32 devices in a mesh: depth: 4 (over z), imgx: 4 (over y, core), imgy: 2 (over x).
Axes of the slice: x: 2, y: 2, z: 4, core: 2. Of those that a mesh axis runs over, the one named last changes fastest.
Arguments:
- emissivity: bfloat16 [32, 512, 256], P('depth', 'imgx', 'imgy'), may hold values from 0.099609375 to 10
- bin_index: int32 [32, 512, 256], P('depth', 'imgx', 'imgy'), may hold values from 0 to 127
- color_table: bfloat16 [4, 128], replicated, may hold values from 0.049804688 to 1
- brick_order: int32 [4], replicated, may hold values from 0 to 3, each once
Outputs:
- image: float32 [4, 512, 256], P(None, 'imgx', 'imgy')
The draws below stay inside these ranges and needn't reach their ends.
Inputs may be any that keep to these rules, and one draw needn't show every extreme that they name: brick_order names every brick index once.
All inputs are finite; a program needn't handle non-finite values.
Results may differ from the reference program's by a relative error of at most 0.0003.
Values sent between devices are 32-bit elements; how exact they have to be, the bound alone decides.
A program may use at most 64 MiB of HBM per device.

```python
import math
import jax
import jax.numpy as jnp
from jax import lax

DZ = 8
BINS = 128
NZ = 32
NX = 512
NY = 256
N_DEPTH = 4


def set_ends(entries, rng, least, high):
    extent = entries.shape
    index_at = [jax.random.randint(jax.random.fold_in(rng, axis), (), 0, extent[axis]) for axis in range(len(extent))]
    entries = entries.at[tuple(index_at)].set(least)
    longest = extent.index(max(extent))
    index_at[longest] = (index_at[longest] + 1) % extent[longest]
    return entries.at[tuple(index_at)].set(high)


def level_of(rng, shape, split, least, largest):
    level = 1.0
    for dim, shards_of in split:
        heights = jax.random.uniform(jax.random.fold_in(jax.random.fold_in(rng, 6), dim), (shards_of,), jnp.float32, least / len(split), largest / len(split))
        level = level * jnp.repeat(jnp.exp(heights), shape[dim] // shards_of).reshape((-1,) + (1,) * (len(shape) - 1 - dim))
    return level


def setup_inputs(seed: int = 0) -> dict:
    keys = jax.random.split(jax.random.key(seed), 5)
    emissivity = jnp.clip(jnp.exp(math.log(10.0) - 4.609084 * jax.random.uniform(keys[0], (NZ, NX, NY), jnp.float32) ** level_of(keys[0], (NZ, NX, NY), ((0, 4), (1, 4), (2, 2)), -0.2, 0.2)), 0.099609375, 10.0).astype(jnp.bfloat16)
    bin_index = set_ends(jax.random.randint(keys[1], (NZ, NX, NY), 0, BINS), jax.random.fold_in(keys[1], 1), 0, BINS - 1).astype(jnp.int32)
    color_table = jnp.clip(jnp.exp(jax.random.uniform(keys[2], (4, BINS), jnp.float32, math.log(0.049804688), math.log(1.0))), 0.049804688, 1.0).astype(jnp.bfloat16)
    brick_order = jax.random.permutation(keys[3], N_DEPTH).astype(jnp.int32)
    return dict(emissivity=emissivity, bin_index=bin_index, color_table=color_table, brick_order=brick_order)


def brick_partial(bright_cells, bin_cells, color_table, ray_step):
    looked = color_table.astype(jnp.float32)[:, bin_cells]
    bright = bright_cells.astype(jnp.float32)
    glow_rgb = bright[None] * looked[0:3]
    absorb_rate = bright * looked[3]
    depth_in = jnp.cumsum(absorb_rate, axis=0) - absorb_rate
    light_in = jnp.exp(-ray_step * depth_in)
    color_sum = jnp.sum(ray_step * glow_rgb * light_in[None], axis=1)
    passed = jnp.exp(-ray_step * jnp.sum(absorb_rate, axis=0))
    return color_sum, passed


def reference(emissivity, bin_index, color_table, brick_order):
    ray_step = 2.0 / NZ

    def advance(state_pair, brick_id):
        color_acc, through = state_pair
        start_cell = (brick_id * DZ).astype(jnp.int32)
        brick_cells = lax.dynamic_slice_in_dim(emissivity, start_cell, DZ, 0)
        brick_bins = lax.dynamic_slice_in_dim(bin_index, start_cell, DZ, 0)
        color_sum, passed = brick_partial(brick_cells, brick_bins, color_table, ray_step)
        return (color_acc + through[None] * color_sum, through * passed), None

    start_state = (jnp.zeros((3, NX, NY), jnp.float32), jnp.ones((NX, NY), jnp.float32))
    final_state, _ = lax.scan(advance, start_state, brick_order)
    color_acc, through = final_state
    return jnp.concatenate([color_acc, (1.0 - through)[None]], 0)
```

```python
import functools

import jax
import jax.numpy as jnp
from jax import lax
from jax.experimental import pallas as pl
from jax.experimental.pallas import tpu as pltpu
from jax.sharding import PartitionSpec as P

MESH = pl.DeviceIdType.MESH
BLOCK = 8
LANES = 128
GROUP = 4
RS = (((3,), (2,), (1,), (0,)), ((3,), (2,), (0,), (1,)), ((0, 1), (3,), (2,)), ((0, 1), (2,), (3,)))
RELAY_ORDER = ((3, 0), (2, 1))
DIRECT = (2,)


def look(channel_tables, bins):
    slabs = len(channel_tables[0])
    if slabs == 1:
        return [jnp.take_along_axis(t[0], bins, axis=1, mode="promise_in_bounds") for t in channel_tables]
    within = bins % LANES
    slab_of = bins // LANES
    out = []
    for t in channel_tables:
        value = jnp.take_along_axis(t[0], within, axis=1, mode="promise_in_bounds")
        for s in range(1, slabs):
            other = jnp.take_along_axis(t[s], within, axis=1, mode="promise_in_bounds")
            value = jnp.where(slab_of == s, other, value)
        out.append(value)
    return out


def scaled_tables(table_ref, ray_step):
    table = table_ref[...].astype(jnp.float32) * ray_step
    slabs = table.shape[1] // LANES
    return [
        [jnp.broadcast_to(table[c : c + 1, s * LANES : (s + 1) * LANES], (BLOCK, LANES)) for s in range(slabs)]
        for c in range(4)
    ]


def march(tables, emis_ref, bins_ref, start):
    cells = emis_ref.shape[0]
    rows = pl.ds(start, BLOCK)
    color = [None] * 3
    depth_in = None
    for z in range(cells):
        bright = emis_ref[z, rows, :].astype(jnp.float32)
        looked = look(tables, bins_ref[z, rows, :])
        rate = bright * looked[3]
        if depth_in is None:
            color = [bright * looked[c] for c in range(3)]
            depth_in = rate
        else:
            seen = bright * jnp.exp(-depth_in)
            color = [color[c] + seen * looked[c] for c in range(3)]
            depth_in = depth_in + rate
    return color + [jnp.exp(-depth_in)]


def pick(options, me):
    value = jnp.int32(options[0])
    for i in range(1, len(options)):
        value = jnp.where(me == i, jnp.int32(options[i]), value)
    return value


def owned_sizes(blocks):
    quarter, shift = blocks // 4, blocks // 16
    return (quarter, quarter, quarter + shift, quarter - shift)


def owned_blocks(sizes, groups):
    steps = []
    for group in groups:
        woven = [((k + 0.5) / sizes[o], i, o, k) for i, o in enumerate(group) for k in range(sizes[o])]
        steps += [(o, k) for _, _, o, k in sorted(woven)]
    return steps


def either(me, members):
    return functools.reduce(jnp.logical_or, [me == m for m in members], False)


def fused(n, ray_step, emis_hbm, bins_hbm, table_in, order_in, out_ref,
          emis, bins, outgoing, arrived, mine, table_v, order_s, in_sem, aux_sem,
          send_sem, recv_sem, give_sem, take_sem, cross_sem, relay_sem, ready_sem):
    me = lax.axis_index("depth")
    y = lax.axis_index("imgx")
    core = lax.rem(y, 2)
    leaf, hub = core == 0, core == 1
    leaf_y, hub_y = y - core, y - core + 1
    blocks = emis.shape[0]
    half = n // 2
    sizes = owned_sizes(blocks)
    offs = [sum(sizes[:m]) for m in range(n)]
    plan = [owned_blocks(sizes, RS[m]) for m in range(n)]

    def at_leaf(d):
        return {"depth": d, "imgx": leaf_y}

    def at_hub(d):
        return {"depth": d, "imgx": hub_y}

    barrier = pltpu.get_barrier_semaphore()

    @pl.when(hub)
    def _():
        for h in range(1, n):
            pl.semaphore_signal(barrier, inc=1, device_id=at_hub(lax.rem(me + h, n)), device_id_type=MESH)
        for h in range(n):
            pl.semaphore_signal(barrier, inc=1, device_id=at_leaf(lax.rem(me + h, n)), device_id_type=MESH)

    def block_rows(block):
        return pl.ds(pl.multiple_of(block * BLOCK, BLOCK), BLOCK)

    owner = [pick([plan[m][q][0] for m in range(n)], me) for q in range(blocks)]
    place = [pick([plan[m][q][1] for m in range(n)], me) for q in range(blocks)]
    block = [pick([offs[plan[m][q][0]] + plan[m][q][1] for m in range(n)], me) for q in range(blocks)]
    first_own = pick(offs, me)
    group = blocks // GROUP

    for q in range(blocks):
        src = block_rows(block[q])
        pltpu.make_async_copy(emis_hbm.at[:, src, :], emis.at[q], in_sem.at[0, q // group]).start()
        pltpu.make_async_copy(bins_hbm.at[:, src, :], bins.at[q], in_sem.at[1, q // group]).start()
        if q == group - 1:
            tc = pltpu.make_async_copy(table_in, table_v, aux_sem.at[0])
            oc = pltpu.make_async_copy(order_in, order_s, aux_sem.at[1])
            tc.start()
            oc.start()
    tc.wait()
    tables = scaled_tables(table_v, ray_step)

    def ship(q):
        pltpu.make_async_remote_copy(
            src_ref=outgoing.at[q],
            dst_ref=arrived.at[core, place[q], me],
            send_sem=send_sem,
            recv_sem=recv_sem.at[core, place[q]],
            device_id=at_hub(owner[q]),
            device_id_type=MESH,
        ).start()

    for q in range(blocks):
        if q % group == 0:
            part = pl.ds(q, group)
            pltpu.make_async_copy(emis.at[part], emis.at[part], in_sem.at[0, q // group]).wait()
            pltpu.make_async_copy(bins.at[part], bins.at[part], in_sem.at[1, q // group]).wait()
        got = march(tables, emis.at[q], bins.at[q], 0)
        for c in range(4):
            outgoing[q, c, :, :] = got[c]
        if q == 0:
            pl.semaphore_wait(barrier, jnp.where(hub, n - 1, n))

            @pl.when(leaf)
            def _():
                for h in range(n):
                    pl.semaphore_signal(ready_sem, inc=1, device_id=at_hub(lax.rem(me + h, n)), device_id_type=MESH)
        stays = [m for m in range(n) if plan[m][q][0] == m]
        if not stays:
            ship(q)
        else:
            here = jnp.logical_and(hub, either(me, stays))

            @pl.when(here)
            def _():
                arrived[1, place[q], me] = outgoing[q]

            @pl.when(jnp.logical_not(here))
            def _():
                ship(q)

    oc.wait()
    own_count = pick(sizes, me)
    cross = jnp.where(me < half, half, 0)
    partner = me + 1 - 2 * lax.rem(me, 2)
    cross_slot = jnp.where(me < half, me, n - 1 - me)
    direct = either(me, DIRECT)

    def span_bytes(ref, sem, other):
        return pltpu.make_async_remote_copy(src_ref=ref, dst_ref=ref, send_sem=sem, recv_sem=other, device_id=at_hub(me), device_id_type=MESH)

    def give(k, tile, d, sem):
        pltpu.make_async_remote_copy(
            src_ref=mine.at[tile, k],
            dst_ref=out_ref.at[:, block_rows(first_own + k), :],
            send_sem=give_sem,
            recv_sem=sem,
            device_id=at_leaf(d) if tile == 0 else at_hub(d),
            device_id_type=MESH,
        ).start()

    @pl.when(hub)
    def _():
        pl.semaphore_wait(ready_sem, n)
        rank = [sum(jnp.where(order_s[q] == m, q, 0) for q in range(n)) for m in range(n)]
        before = [[rank[a] < rank[b] for b in range(n)] for a in range(n)]

        def settle(k, tile):
            span_bytes(arrived.at[tile, 0, pl.ds(0, n - tile)], send_sem, recv_sem.at[tile, k]).wait_recv()
            passed = [arrived[tile, k, m, 3] for m in range(n)]
            through = functools.reduce(lambda u, v: u * v, passed)
            color = [0.0] * 3
            for b in range(n):
                ahead = None
                for a in range(n):
                    if a != b:
                        factor = jnp.where(before[a][b], passed[a], 1.0)
                        ahead = factor if ahead is None else ahead * factor
                color = [color[c] + ahead * arrived[tile, k, b, c] for c in range(3)]
            for c in range(3):
                mine[tile, k, c] = color[c]
            mine[tile, k, 3] = 1.0 - through

        def chunk(k, carry):
            for tile in range(2):
                settle(k, tile)
                give(k, tile, cross, cross_sem.at[cross_slot, k])
                give(k, tile, partner, take_sem)
                if tile == 0:
                    give(k, tile, me, take_sem)
            return carry

        lax.fori_loop(0, own_count, chunk, 0)
        if DIRECT:
            @pl.when(direct)
            def _():
                def more(k, carry):
                    for tile in range(2):
                        give(k, tile, cross + 1, take_sem)
                    return carry
                lax.fori_loop(0, own_count, more, 0)

        def keep(k, carry):
            out_ref[:, block_rows(first_own + k), :] = mine[1, k]
            return carry

        lax.fori_loop(0, own_count, keep, 0)

    even = lax.rem(me, 2) == 0

    @pl.when(even)
    def _():
        for left_far, right_far in RELAY_ORDER:
            both = (left_far, right_far)
            far = pick([left_far] * half + [right_far] * half, me)
            begin = pick([offs[left_far]] * half + [offs[right_far]] * half, me)
            count = pick([sizes[left_far]] * half + [sizes[right_far]] * half, me)
            slot = pick([n - 1 - left_far] * half + [right_far] * half, me)
            handed = [m for m in both if m not in DIRECT]

            def relay(k, carry):
                spot = out_ref.at[:, block_rows(begin + k), :]
                span_bytes(spot, relay_sem, cross_sem.at[slot, k]).wait_recv()

                @pl.when(either(far, handed))
                def _():
                    pltpu.make_async_remote_copy(
                        src_ref=spot, dst_ref=spot, send_sem=relay_sem, recv_sem=take_sem,
                        device_id={"depth": me + 1}, device_id_type=MESH).start()
                return carry

            lax.fori_loop(0, count, relay, 0)

    def rows_of(count):
        return out_ref.at[:, pl.ds(0, count * BLOCK), :]

    for m in range(n):
        cross_owners = [o for o in range(n) if (o < half) != (m < half)]
        near = [o for o in range(n) if (o < half) == (m < half)]
        into = near if m % 2 == 0 else list(range(n))
        with_direct = [o for o in cross_owners if m % 2 == 0 and o not in DIRECT]

        @pl.when(jnp.logical_and(me == m, leaf))
        def _():
            span_bytes(outgoing, send_sem, take_sem).wait_send()
            span_bytes(rows_of(sum(sizes[o] for o in into)), give_sem, take_sem).wait_recv()

        @pl.when(jnp.logical_and(me == m, hub))
        def _():
            span_bytes(outgoing.at[pl.ds(0, blocks - sizes[m])], send_sem, take_sem).wait_send()
            span_bytes(rows_of(sum(sizes[o] for o in into) - sizes[m]), give_sem, take_sem).wait_recv()
            for _ in range(7 if m in DIRECT else 5):
                span_bytes(rows_of(sizes[m]), give_sem, take_sem).wait_send()
        if with_direct:
            @pl.when(me == m)
            def _():
                span_bytes(rows_of(sum(sizes[o] for o in with_direct)), relay_sem, take_sem).wait_send()


def fused_call(emissivity, bin_index, color_table, brick_order, n, ray_step):
    cells, cols_x, cols_y = emissivity.shape
    blocks = cols_x // BLOCK
    most = max(owned_sizes(blocks))
    return pl.pallas_call(
        functools.partial(fused, n, ray_step),
        out_shape=pltpu.VMEM((4, cols_x, cols_y), jnp.float32),
        in_specs=[pl.BlockSpec(memory_space=pltpu.HBM)] * 4,
        out_specs=pl.BlockSpec(memory_space=pltpu.VMEM),
        scratch_shapes=[
            pltpu.VMEM((blocks, cells, BLOCK, cols_y), jnp.bfloat16),
            pltpu.VMEM((blocks, cells, BLOCK, cols_y), jnp.int32),
            pltpu.VMEM((blocks, 4, BLOCK, cols_y), jnp.float32),
            pltpu.VMEM((2, most, n, 4, BLOCK, cols_y), jnp.float32),
            pltpu.VMEM((2, most, 4, BLOCK, cols_y), jnp.float32),
            pltpu.VMEM(color_table.shape, color_table.dtype),
            pltpu.SMEM(brick_order.shape, brick_order.dtype),
            pltpu.SemaphoreType.DMA((2, GROUP)),
            pltpu.SemaphoreType.DMA((2,)),
            pltpu.SemaphoreType.DMA(()),
            pltpu.SemaphoreType.DMA((2, most)),
            pltpu.SemaphoreType.DMA(()),
            pltpu.SemaphoreType.DMA(()),
            pltpu.SemaphoreType.DMA((2, most)),
            pltpu.SemaphoreType.DMA(()),
            pltpu.SemaphoreType.REGULAR,
        ],
        compiler_params=pltpu.CompilerParams(collective_id=0, has_side_effects=True),
    )(emissivity, bin_index, color_table, brick_order)


def march_kernel(ray_step, emis_ref, bins_ref, table_ref, out_ref):
    tables = scaled_tables(table_ref, ray_step)

    @pl.loop(0, emis_ref.shape[1] // BLOCK)
    def _(r):
        start = pl.multiple_of(r * BLOCK, BLOCK)
        part = march(tables, emis_ref, bins_ref, start)
        for c in range(4):
            out_ref[c, pl.ds(start, BLOCK), :] = part[c]


def spread(emissivity, bin_index, color_table, brick_order, n, ray_step):
    cells, cols_x, cols_y = emissivity.shape
    piece_len = cols_x * cols_y // n
    stacked = pl.pallas_call(
        functools.partial(march_kernel, ray_step),
        out_shape=jax.ShapeDtypeStruct((4, cols_x, cols_y), jnp.float32),
        in_specs=[pl.BlockSpec(memory_space=pltpu.VMEM)] * 3,
        out_specs=pl.BlockSpec(memory_space=pltpu.VMEM),
    )(emissivity, bin_index, color_table)
    stacked = stacked.reshape(1, 4, n, piece_len).transpose(2, 0, 1, 3).reshape(n, 4, piece_len)
    received = lax.all_to_all(stacked, "depth", split_axis=0, concat_axis=0, tiled=True)
    ordered = jnp.take(received, brick_order, axis=0)
    color, through = ordered[0, 0:3], ordered[0, 3]
    for k in range(1, n):
        color = color + through * ordered[k, 0:3]
        through = through * ordered[k, 3]
    piece = jnp.concatenate([color, (1.0 - through)[None]], 0)
    return lax.all_gather(piece, "depth", axis=1, tiled=True).reshape(4, cols_x, cols_y)


def on_device(emissivity, bin_index, color_table, brick_order):
    cells, cols_x, cols_y = emissivity.shape
    n = lax.axis_size("depth")
    ray_step = 2.0 / (cells * n)
    paired = lax.axis_size("imgx") % 2 == 0
    piecewise = n == len(RS) and paired and cols_x % (4 * n * BLOCK) == 0
    form = fused_call if piecewise else spread
    return form(emissivity, bin_index, color_table, brick_order, n, ray_step)


def solution(mesh):
    return jax.shard_map(
        on_device,
        mesh=mesh,
        in_specs=(P("depth", "imgx", "imgy"), P("depth", "imgx", "imgy"), P(), P()),
        out_specs=P(None, "imgx", "imgy"),
        check_vma=False,
    )
```

```python
import functools

import jax
import jax.numpy as jnp
from jax import lax
from jax.experimental import pallas as pl
from jax.experimental.pallas import tpu as pltpu
from jax.sharding import PartitionSpec as P

MESH = pl.DeviceIdType.MESH
BLOCK = 8
LANES = 128
MEET = 12
GROUP = 4
RS = (((1,), (2,), (3,), (0,)), ((0,), (2,), (3,), (1,)), ((0, 1), (3,), (2,)), ((2, 0, 1), (3,)))
RELAY_ORDER = ((3, 0), (2, 1))
DIRECT = (1, 1, 4, 0)
SIZES = (4, 4, 8, 0)


def look(channel_tables, bins):
    slabs = len(channel_tables[0])
    if slabs == 1:
        return [jnp.take_along_axis(t[0], bins, axis=1, mode="promise_in_bounds") for t in channel_tables]
    within = bins % LANES
    slab_of = bins // LANES
    out = []
    for t in channel_tables:
        value = jnp.take_along_axis(t[0], within, axis=1, mode="promise_in_bounds")
        for s in range(1, slabs):
            other = jnp.take_along_axis(t[s], within, axis=1, mode="promise_in_bounds")
            value = jnp.where(slab_of == s, other, value)
        out.append(value)
    return out


def scaled_tables(table_ref, ray_step):
    table = table_ref[...].astype(jnp.float32) * ray_step
    slabs = table.shape[1] // LANES
    return [
        [jnp.broadcast_to(table[c : c + 1, s * LANES : (s + 1) * LANES], (BLOCK, LANES)) for s in range(slabs)]
        for c in range(4)
    ]


def march(tables, emis_ref, bins_ref, start):
    cells = emis_ref.shape[0]
    rows = pl.ds(start, BLOCK)
    color = [None] * 3
    depth_in = None
    for z in range(cells):
        bright = emis_ref[z, rows, :].astype(jnp.float32)
        looked = look(tables, bins_ref[z, rows, :])
        rate = bright * looked[3]
        if depth_in is None:
            color = [bright * looked[c] for c in range(3)]
            depth_in = rate
        else:
            seen = bright * jnp.exp(-depth_in)
            color = [color[c] + seen * looked[c] for c in range(3)]
            depth_in = depth_in + rate
    return color + [jnp.exp(-depth_in)]


def pick(options, me):
    value = jnp.int32(options[0])
    for i in range(1, len(options)):
        value = jnp.where(me == i, jnp.int32(options[i]), value)
    return value


def scaled(shares, blocks):
    return tuple(share * blocks // sum(SIZES) for share in shares)


def owned_blocks(sizes, groups):
    steps = []
    for group in groups:
        woven = [((k + 0.5) / sizes[o], i, o, k) for i, o in enumerate(group) for k in range(sizes[o])]
        steps += [(o, k) for _, _, o, k in sorted(woven)]
    return steps


def either(me, members):
    return functools.reduce(jnp.logical_or, [me == m for m in members], False)


def fused(n, ray_step, emis_hbm, bins_hbm, table_in, order_in, out_ref,
          emis, bins, outgoing, arrived, mine, table_v, order_s, in_sem, aux_sem,
          send_sem, recv_sem, give_sem, take_sem, cross_sem, relay_sem, ready_sem, know_sem, leaf_sem):
    me = lax.axis_index("depth")
    y = lax.axis_index("imgx")
    core = lax.rem(y, 2)
    leaf, hub = core == 0, core == 1
    leaf_y, hub_y = y - core, y - core + 1
    blocks = emis.shape[0]
    half = n // 2
    sizes, direct_of = scaled(SIZES, blocks), scaled(DIRECT, blocks)
    offs = [sum(sizes[:m]) for m in range(n)]
    plan = [owned_blocks(sizes, RS[m]) for m in range(n)]

    def at_leaf(d):
        return {"depth": d, "imgx": leaf_y}

    def at_hub(d):
        return {"depth": d, "imgx": hub_y}

    barrier = pltpu.get_barrier_semaphore()

    @pl.when(hub)
    def _():
        pl.semaphore_signal(barrier, inc=1, device_id=at_leaf(me), device_id_type=MESH)
        for d in range(n):
            @pl.when((d > me) | ((d == 0) & (me == 1)))
            def _():
                pl.semaphore_signal(barrier, inc=1, device_id=at_hub(d), device_id_type=MESH)

    def block_rows(block):
        return pl.ds(pl.multiple_of(block * BLOCK, BLOCK), BLOCK)

    owner = [pick([plan[m][q][0] for m in range(n)], me) for q in range(blocks)]
    place = [pick([plan[m][q][1] for m in range(n)], me) for q in range(blocks)]
    block = [pick([offs[plan[m][q][0]] + plan[m][q][1] for m in range(n)], me) for q in range(blocks)]
    first_own = pick(offs, me)
    group = blocks // GROUP

    for q in range(blocks):
        src = block_rows(block[q])
        pltpu.make_async_copy(emis_hbm.at[:, src, :], emis.at[q], in_sem.at[0, q // group]).start()
        pltpu.make_async_copy(bins_hbm.at[:, src, :], bins.at[q], in_sem.at[1, q // group]).start()
        if q == group - 1:
            tc = pltpu.make_async_copy(table_in, table_v, aux_sem.at[0])
            oc = pltpu.make_async_copy(order_in, order_s, aux_sem.at[1])
            tc.start()
            oc.start()
    pl.semaphore_wait(barrier, jnp.where(hub, jnp.maximum(me, 1), 1))

    @pl.when(hub)
    def _():
        for d in range(n):
            @pl.when(d < me)
            def _():
                pl.semaphore_signal(know_sem.at[me], inc=1, device_id=at_hub(d), device_id_type=MESH)
        pl.semaphore_wait(leaf_sem, 1)
        for d in range(n):
            @pl.when(d < me)
            def _():
                pl.semaphore_signal(know_sem.at[d], inc=1, device_id=at_leaf(me), device_id_type=MESH)

    @pl.when(leaf)
    def _():
        pl.semaphore_signal(leaf_sem, inc=1, device_id=at_hub(me), device_id_type=MESH)

    def meet(t):
        @pl.when(jnp.logical_and(hub, t > me))
        def _():
            pl.semaphore_wait(know_sem.at[t], 1)
            pl.semaphore_signal(know_sem.at[t], inc=1, device_id=at_leaf(me), device_id_type=MESH)

        @pl.when(jnp.logical_and(leaf, t != me))
        def _():
            pl.semaphore_wait(know_sem.at[t], 1)

    tc.wait()
    tables = scaled_tables(table_v, ray_step)

    def ship(q):
        pltpu.make_async_remote_copy(
            src_ref=outgoing.at[q],
            dst_ref=arrived.at[core, place[q], me],
            send_sem=send_sem,
            recv_sem=recv_sem.at[core, place[q]],
            device_id=at_hub(owner[q]),
            device_id_type=MESH,
        ).start()

    last_meet = blocks * MEET // sum(SIZES)
    for q in range(blocks):
        if q % group == 0:
            part = pl.ds(q, group)
            pltpu.make_async_copy(emis.at[part], emis.at[part], in_sem.at[0, q // group]).wait()
            pltpu.make_async_copy(bins.at[part], bins.at[part], in_sem.at[1, q // group]).wait()
        got = march(tables, emis.at[q], bins.at[q], 0)
        for c in range(4):
            outgoing[q, c, :, :] = got[c]
        fresh = [m for m in range(n) if plan[m][q][0] not in [o for o, _ in plan[m][:q]]]
        if fresh:
            @pl.when(either(me, fresh))
            def _():
                meet(owner[q])
        if q == last_meet:
            for t in range(n):
                unmet = [m for m in range(n) if m != t and t not in [o for o, _ in plan[m]]]
                if unmet:
                    @pl.when(either(me, unmet))
                    def _():
                        meet(jnp.int32(t))
            @pl.when(leaf)
            def _():
                for h in range(n):
                    pl.semaphore_signal(ready_sem, inc=1, device_id=at_hub(lax.rem(me + h, n)), device_id_type=MESH)
        stays = [m for m in range(n) if plan[m][q][0] == m]
        if not stays:
            ship(q)
        else:
            here = jnp.logical_and(hub, either(me, stays))

            @pl.when(here)
            def _():
                arrived[1, place[q], me] = outgoing[q]

            @pl.when(jnp.logical_not(here))
            def _():
                ship(q)

    oc.wait()
    own_count = pick(sizes, me)
    cross = jnp.where(me < half, half, 0)
    partner = me + 1 - 2 * lax.rem(me, 2)
    cross_slot = jnp.where(me < half, me, n - 1 - me)
    direct = pick(direct_of, me)

    def span_bytes(ref, sem, other):
        return pltpu.make_async_remote_copy(src_ref=ref, dst_ref=ref, send_sem=sem, recv_sem=other, device_id=at_hub(me), device_id_type=MESH)

    def give(k, tile, d, sem):
        pltpu.make_async_remote_copy(
            src_ref=mine.at[tile, k],
            dst_ref=out_ref.at[:, block_rows(first_own + k), :],
            send_sem=give_sem,
            recv_sem=sem,
            device_id=at_leaf(d) if tile == 0 else at_hub(d),
            device_id_type=MESH,
        ).start()

    @pl.when(hub)
    def _():
        pl.semaphore_wait(ready_sem, n)
        rank = [sum(jnp.where(order_s[q] == m, q, 0) for q in range(n)) for m in range(n)]
        before = [[rank[a] < rank[b] for b in range(n)] for a in range(n)]

        def settle(k, tile):
            span_bytes(arrived.at[tile, 0, pl.ds(0, n - tile)], send_sem, recv_sem.at[tile, k]).wait_recv()
            passed = [arrived[tile, k, m, 3] for m in range(n)]
            through = functools.reduce(lambda u, v: u * v, passed)
            color = [0.0] * 3
            for b in range(n):
                ahead = None
                for a in range(n):
                    if a != b:
                        factor = jnp.where(before[a][b], passed[a], 1.0)
                        ahead = factor if ahead is None else ahead * factor
                color = [color[c] + ahead * arrived[tile, k, b, c] for c in range(3)]
            for c in range(3):
                mine[tile, k, c] = color[c]
            mine[tile, k, 3] = 1.0 - through

        def chunk(k, carry):
            for tile in range(2):
                settle(k, tile)
                give(k, tile, cross, cross_sem.at[cross_slot, k])
                give(k, tile, partner, take_sem)
                if tile == 0:
                    give(k, tile, me, take_sem)
            return carry

        lax.fori_loop(0, own_count, chunk, 0)
        if any(direct_of):
            def more(k, carry):
                for tile in range(2):
                    give(k, tile, cross + 1, take_sem)
                return carry
            lax.fori_loop(own_count - direct, own_count, more, 0)

        def keep(k, carry):
            out_ref[:, block_rows(first_own + k), :] = mine[1, k]
            return carry

        lax.fori_loop(0, own_count, keep, 0)

    even = lax.rem(me, 2) == 0

    @pl.when(even)
    def _():
        for left_far, right_far in RELAY_ORDER:
            both = (left_far, right_far)
            begin = pick([offs[left_far]] * half + [offs[right_far]] * half, me)
            count = pick([sizes[left_far]] * half + [sizes[right_far]] * half, me)
            slot = pick([n - 1 - left_far] * half + [right_far] * half, me)
            handed = count - pick([direct_of[left_far]] * half + [direct_of[right_far]] * half, me)

            def relay(k, carry):
                spot = out_ref.at[:, block_rows(begin + k), :]
                span_bytes(spot, relay_sem, cross_sem.at[slot, k]).wait_recv()

                @pl.when(k < handed)
                def _():
                    pltpu.make_async_remote_copy(
                        src_ref=spot, dst_ref=spot, send_sem=relay_sem, recv_sem=take_sem,
                        device_id={"depth": me + 1}, device_id_type=MESH).start()
                return carry

            lax.fori_loop(0, count, relay, 0)

    def rows_of(count):
        return out_ref.at[:, pl.ds(0, count * BLOCK), :]

    def await_rows(count, sent, sem):
        if count:
            wait = span_bytes(rows_of(count), sem, sem)
            (wait.wait_send if sent else wait.wait_recv)()

    for m in range(n):
        near = [o for o in range(n) if (o < half) == (m < half)]
        far = [o for o in range(n) if o not in near]
        into = near if m % 2 == 0 else list(range(n))
        received = sum(sizes[o] for o in into)
        relayed = sum(sizes[o] - direct_of[o] for o in far) if m % 2 == 0 else 0

        @pl.when(jnp.logical_and(me == m, leaf))
        def _():
            span_bytes(outgoing, send_sem, send_sem).wait_send()
            await_rows(received, False, take_sem)

        @pl.when(jnp.logical_and(me == m, hub))
        def _():
            span_bytes(outgoing.at[pl.ds(0, blocks - sizes[m])], send_sem, send_sem).wait_send()
            await_rows(received - sizes[m], False, take_sem)
            for _ in range(5):
                await_rows(sizes[m], True, give_sem)
            for _ in range(2):
                await_rows(direct_of[m], True, give_sem)
        if relayed:
            @pl.when(me == m)
            def _():
                await_rows(relayed, True, relay_sem)


def fused_call(emissivity, bin_index, color_table, brick_order, n, ray_step):
    cells, cols_x, cols_y = emissivity.shape
    blocks = cols_x // BLOCK
    most = max(scaled(SIZES, blocks))
    return pl.pallas_call(
        functools.partial(fused, n, ray_step),
        out_shape=pltpu.VMEM((4, cols_x, cols_y), jnp.float32),
        in_specs=[pl.BlockSpec(memory_space=pltpu.HBM)] * 4,
        out_specs=pl.BlockSpec(memory_space=pltpu.VMEM),
        scratch_shapes=[
            pltpu.VMEM((blocks, cells, BLOCK, cols_y), jnp.bfloat16),
            pltpu.VMEM((blocks, cells, BLOCK, cols_y), jnp.int32),
            pltpu.VMEM((blocks, 4, BLOCK, cols_y), jnp.float32),
            pltpu.VMEM((2, most, n, 4, BLOCK, cols_y), jnp.float32),
            pltpu.VMEM((2, most, 4, BLOCK, cols_y), jnp.float32),
            pltpu.VMEM(color_table.shape, color_table.dtype),
            pltpu.SMEM(brick_order.shape, brick_order.dtype),
            pltpu.SemaphoreType.DMA((2, GROUP)),
            pltpu.SemaphoreType.DMA((2,)),
            pltpu.SemaphoreType.DMA(()),
            pltpu.SemaphoreType.DMA((2, most)),
            pltpu.SemaphoreType.DMA(()),
            pltpu.SemaphoreType.DMA(()),
            pltpu.SemaphoreType.DMA((2, most)),
            pltpu.SemaphoreType.DMA(()),
            pltpu.SemaphoreType.REGULAR,
            pltpu.SemaphoreType.REGULAR((n,)),
            pltpu.SemaphoreType.REGULAR,
        ],
        compiler_params=pltpu.CompilerParams(collective_id=0, has_side_effects=True),
    )(emissivity, bin_index, color_table, brick_order)


def march_kernel(ray_step, emis_ref, bins_ref, table_ref, out_ref):
    tables = scaled_tables(table_ref, ray_step)

    @pl.loop(0, emis_ref.shape[1] // BLOCK)
    def _(r):
        start = pl.multiple_of(r * BLOCK, BLOCK)
        part = march(tables, emis_ref, bins_ref, start)
        for c in range(4):
            out_ref[c, pl.ds(start, BLOCK), :] = part[c]


def spread(emissivity, bin_index, color_table, brick_order, n, ray_step):
    cells, cols_x, cols_y = emissivity.shape
    piece_len = cols_x * cols_y // n
    stacked = pl.pallas_call(
        functools.partial(march_kernel, ray_step),
        out_shape=jax.ShapeDtypeStruct((4, cols_x, cols_y), jnp.float32),
        in_specs=[pl.BlockSpec(memory_space=pltpu.VMEM)] * 3,
        out_specs=pl.BlockSpec(memory_space=pltpu.VMEM),
    )(emissivity, bin_index, color_table)
    stacked = stacked.reshape(1, 4, n, piece_len).transpose(2, 0, 1, 3).reshape(n, 4, piece_len)
    received = lax.all_to_all(stacked, "depth", split_axis=0, concat_axis=0, tiled=True)
    ordered = jnp.take(received, brick_order, axis=0)
    color, through = ordered[0, 0:3], ordered[0, 3]
    for k in range(1, n):
        color = color + through * ordered[k, 0:3]
        through = through * ordered[k, 3]
    piece = jnp.concatenate([color, (1.0 - through)[None]], 0)
    return lax.all_gather(piece, "depth", axis=1, tiled=True).reshape(4, cols_x, cols_y)


def on_device(emissivity, bin_index, color_table, brick_order):
    cells, cols_x, cols_y = emissivity.shape
    n = lax.axis_size("depth")
    ray_step = 2.0 / (cells * n)
    paired = lax.axis_size("imgx") % 2 == 0
    piecewise = n == len(RS) and paired and cols_x % (sum(SIZES) * BLOCK) == 0
    form = fused_call if piecewise else spread
    return form(emissivity, bin_index, color_table, brick_order, n, ray_step)


def solution(mesh):
    return jax.shard_map(
        on_device,
        mesh=mesh,
        in_specs=(P("depth", "imgx", "imgy"), P("depth", "imgx", "imgy"), P(), P()),
        out_specs=P(None, "imgx", "imgy"),
        check_vma=False,
    )
```

```python
import functools

import jax
import jax.numpy as jnp
from jax import lax
from jax.experimental import pallas as pl
from jax.experimental.pallas import tpu as pltpu
from jax.sharding import PartitionSpec as P

MESH = pl.DeviceIdType.MESH
BLOCK = 8
LANES = 128
MEET = 12
GROUP = 2
RS = (((1, 0, 0.33), (2, 0.34, 1), (0, 2, 3)), ((0, 0, 0.18), (2, 0.34, 1), (1, 2, 3)), ((0, 0, 1), (1, 0, 1), (3, 1, 1.5), (2, 2, 3)), ((0, 0, 1), (1, 0, 0.7), (2, 0, 1), (3, 2, 3)))
RELAY_ORDER = ((2, 0), (3, 1))
DIRECT = (1, 1, 4, 0)
SIZES = (4, 4, 8, 0)


def look(channel_tables, bins):
    slabs = len(channel_tables[0])
    if slabs == 1:
        return [jnp.take_along_axis(t[0], bins, axis=1, mode="promise_in_bounds") for t in channel_tables]
    within = bins % LANES
    slab_of = bins // LANES
    out = []
    for t in channel_tables:
        value = jnp.take_along_axis(t[0], within, axis=1, mode="promise_in_bounds")
        for s in range(1, slabs):
            other = jnp.take_along_axis(t[s], within, axis=1, mode="promise_in_bounds")
            value = jnp.where(slab_of == s, other, value)
        out.append(value)
    return out


def scaled_tables(table_ref, ray_step):
    table = table_ref[...].astype(jnp.float32) * ray_step
    slabs = table.shape[1] // LANES
    return [
        [jnp.broadcast_to(table[c : c + 1, s * LANES : (s + 1) * LANES], (BLOCK, LANES)) for s in range(slabs)]
        for c in range(4)
    ]


def march(tables, emis_ref, bins_ref, start):
    cells = emis_ref.shape[0]
    rows = pl.ds(start, BLOCK)
    color = [None] * 3
    depth_in = None
    for z in range(cells):
        bright = emis_ref[z, rows, :].astype(jnp.float32)
        looked = look(tables, bins_ref[z, rows, :])
        rate = bright * looked[3]
        if depth_in is None:
            color = [bright * looked[c] for c in range(3)]
            depth_in = rate
        else:
            seen = bright * jnp.exp(-depth_in)
            color = [color[c] + seen * looked[c] for c in range(3)]
            depth_in = depth_in + rate
    return color + [jnp.exp(-depth_in)]


def pick(options, me):
    value = jnp.int32(options[0])
    for i in range(1, len(options)):
        value = jnp.where(me == i, jnp.int32(options[i]), value)
    return value


def scaled(shares, blocks):
    return tuple(share * blocks // sum(SIZES) for share in shares)


def owned_blocks(sizes, spans):
    steps = [(begin + (end - begin) * (k + 0.5) / sizes[o], o, k) for o, begin, end in spans for k in range(sizes[o])]
    return [(o, k) for _, o, k in sorted(steps)]


def either(me, members):
    return functools.reduce(jnp.logical_or, [me == m for m in members], False)


def fused(n, ray_step, emis_hbm, bins_hbm, table_in, order_in, out_ref,
          emis, bins, outgoing, arrived, mine, table_v, order_s, in_sem,
          out_sem, recv_sem, take_sem, cross_sem, ready_sem, know_sem):
    me = lax.axis_index("depth")
    y = lax.axis_index("imgx")
    core = lax.rem(y, 2)
    leaf, hub = core == 0, core == 1
    leaf_y, hub_y = y - core, y - core + 1
    blocks = emis.shape[0]
    half = n // 2
    sizes, direct_of = scaled(SIZES, blocks), scaled(DIRECT, blocks)
    offs = [sum(sizes[:m]) for m in range(n)]
    plan = [owned_blocks(sizes, RS[m]) for m in range(n)]

    def at_leaf(d):
        return {"depth": d, "imgx": leaf_y}

    def at_hub(d):
        return {"depth": d, "imgx": hub_y}

    barrier = pltpu.get_barrier_semaphore()

    @pl.when(hub)
    def _():
        pl.semaphore_signal(barrier, inc=1, device_id=at_leaf(me), device_id_type=MESH)
        for d in range(n):
            @pl.when((d > me) | ((d == 0) & (me == 1)))
            def _():
                pl.semaphore_signal(barrier, inc=1, device_id=at_hub(d), device_id_type=MESH)

    def block_rows(block):
        return pl.ds(pl.multiple_of(block * BLOCK, BLOCK), BLOCK)

    owner = [pick([plan[m][q][0] for m in range(n)], me) for q in range(blocks)]
    place = [pick([plan[m][q][1] for m in range(n)], me) for q in range(blocks)]
    block = [pick([offs[plan[m][q][0]] + plan[m][q][1] for m in range(n)], me) for q in range(blocks)]
    first_own = pick(offs, me)
    group = blocks // GROUP

    for q in range(blocks):
        src = block_rows(block[q])
        pltpu.make_async_copy(emis_hbm.at[:, src, :], emis.at[q], in_sem.at[q // group]).start()
        pltpu.make_async_copy(bins_hbm.at[:, src, :], bins.at[q], in_sem.at[q // group]).start()
        if q == group - 1:
            tc = pltpu.make_async_copy(table_in, table_v, in_sem.at[0])
            tc.start()
    oc = pltpu.make_async_copy(order_in, order_s, in_sem.at[GROUP - 1])
    oc.start()

    def await_group(g):
        part = pl.ds(g * group, group)
        pltpu.make_async_copy(emis.at[part], emis.at[part], in_sem.at[g]).wait()
        pltpu.make_async_copy(bins.at[part], bins.at[part], in_sem.at[g]).wait()
        if g == 0:
            tc.wait()
        if g == GROUP - 1:
            oc.wait()

    pl.semaphore_wait(barrier, jnp.where(hub, jnp.maximum(me, 1), 1))

    @pl.when(hub)
    def _():
        for d in range(n):
            @pl.when(d < me)
            def _():
                pl.semaphore_signal(know_sem.at[me], inc=1, device_id=at_hub(d), device_id_type=MESH)
        pl.semaphore_wait(know_sem.at[me], 1)
        for d in range(n):
            @pl.when(d < me)
            def _():
                pl.semaphore_signal(know_sem.at[d], inc=1, device_id=at_leaf(me), device_id_type=MESH)

    @pl.when(leaf)
    def _():
        pl.semaphore_signal(know_sem.at[me], inc=1, device_id=at_hub(me), device_id_type=MESH)

    def meet(t):
        @pl.when(jnp.logical_and(hub, t > me))
        def _():
            pl.semaphore_wait(know_sem.at[t], 1)
            pl.semaphore_signal(know_sem.at[t], inc=1, device_id=at_leaf(me), device_id_type=MESH)

        @pl.when(jnp.logical_and(leaf, t != me))
        def _():
            pl.semaphore_wait(know_sem.at[t], 1)

    await_group(0)
    tables = scaled_tables(table_v, ray_step)

    def ship(q):
        pltpu.make_async_remote_copy(
            src_ref=outgoing.at[q],
            dst_ref=arrived.at[place[q], core * n + me],
            send_sem=out_sem,
            recv_sem=recv_sem.at[place[q]],
            device_id=at_hub(owner[q]),
            device_id_type=MESH,
        ).start()

    met = [next(q for q in range(blocks) if plan[m][q][0] == o) for m in range(n) for o in range(n) if o != m and sizes[o]]
    last_meet = max(blocks * MEET // sum(SIZES), *met)
    for q in range(blocks):
        if q % group == 0 and q:
            await_group(q // group)
        got = march(tables, emis.at[q], bins.at[q], 0)
        for c in range(4):
            outgoing[q, c, :, :] = got[c]
        fresh = [m for m in range(n) if plan[m][q][0] not in [o for o, _ in plan[m][:q]]]
        if fresh:
            @pl.when(either(me, fresh))
            def _():
                meet(owner[q])
        if q == last_meet:
            for t in range(n):
                unmet = [m for m in range(n) if m != t and t not in [o for o, _ in plan[m]]]
                if unmet:
                    @pl.when(either(me, unmet))
                    def _():
                        meet(jnp.int32(t))
            @pl.when(leaf)
            def _():
                for h in range(n):
                    pl.semaphore_signal(ready_sem, inc=1, device_id=at_hub(lax.rem(me + h, n)), device_id_type=MESH)
        stays = [m for m in range(n) if plan[m][q][0] == m]
        if not stays:
            ship(q)
        else:
            here = jnp.logical_and(hub, either(me, stays))

            @pl.when(here)
            def _():
                arrived[place[q], n + me] = outgoing[q]

            @pl.when(jnp.logical_not(here))
            def _():
                ship(q)

    own_count = pick(sizes, me)
    cross = jnp.where(me < half, half, 0)
    partner = me + 1 - 2 * lax.rem(me, 2)
    cross_base = [offs[o] - offs[o // half * half] for o in range(n)]
    cross_at = pick(cross_base, me)
    direct = pick(direct_of, me)

    def span_bytes(ref, sem, other):
        return pltpu.make_async_remote_copy(src_ref=ref, dst_ref=ref, send_sem=sem, recv_sem=other, device_id=at_hub(me), device_id_type=MESH)

    def give(k, tile, d, sem):
        pltpu.make_async_remote_copy(
            src_ref=mine.at[tile, k],
            dst_ref=out_ref.at[:, block_rows(first_own + k), :],
            send_sem=out_sem,
            recv_sem=sem,
            device_id=at_leaf(d) if tile == 0 else at_hub(d),
            device_id_type=MESH,
        ).start()

    @pl.when(hub)
    def _():
        pl.semaphore_wait(ready_sem, n)
        rank = [sum(jnp.where(order_s[q] == m, q, 0) for q in range(n)) for m in range(n)]
        before = [[rank[a] < rank[b] for b in range(n)] for a in range(n)]

        def settle(k, tile):
            passed = [arrived[k, tile * n + m, 3] for m in range(n)]
            through = functools.reduce(lambda u, v: u * v, passed)
            color = [0.0] * 3
            for b in range(n):
                ahead = None
                for a in range(n):
                    if a != b:
                        factor = jnp.where(before[a][b], passed[a], 1.0)
                        ahead = factor if ahead is None else ahead * factor
                color = [color[c] + ahead * arrived[k, tile * n + b, c] for c in range(3)]
            for c in range(3):
                mine[tile, k, c] = color[c]
            mine[tile, k, 3] = 1.0 - through

        def chunk(k, carry):
            span_bytes(arrived.at[0, pl.ds(0, 2 * n - 1)], out_sem, recv_sem.at[k]).wait_recv()
            for tile in range(2):
                settle(k, tile)
                give(k, tile, cross, cross_sem.at[cross_at + k])
                give(k, tile, partner, take_sem)
                if tile == 0:
                    give(k, tile, me, take_sem)
            return carry

        lax.fori_loop(0, own_count, chunk, 0)
        if any(direct_of):
            def more(k, carry):
                for tile in range(2):
                    give(k, tile, cross + 1, take_sem)
                return carry
            lax.fori_loop(own_count - direct, own_count, more, 0)

        def keep(k, carry):
            out_ref[:, block_rows(first_own + k), :] = mine[1, k]
            return carry

        lax.fori_loop(0, own_count, keep, 0)

    even = lax.rem(me, 2) == 0

    @pl.when(even)
    def _():
        for left_far, right_far in RELAY_ORDER:
            both = (left_far, right_far)
            begin = pick([offs[left_far]] * half + [offs[right_far]] * half, me)
            count = pick([sizes[left_far]] * half + [sizes[right_far]] * half, me)
            slot = pick([cross_base[left_far]] * half + [cross_base[right_far]] * half, me)
            handed = count - pick([direct_of[left_far]] * half + [direct_of[right_far]] * half, me)

            def relay(k, carry):
                spot = out_ref.at[:, block_rows(begin + k), :]
                span_bytes(spot, out_sem, cross_sem.at[slot + k]).wait_recv()

                @pl.when(k < handed)
                def _():
                    pltpu.make_async_remote_copy(
                        src_ref=spot, dst_ref=spot, send_sem=out_sem, recv_sem=take_sem,
                        device_id={"depth": me + 1}, device_id_type=MESH).start()
                return carry

            lax.fori_loop(0, count, relay, 0)

    def rows_of(count):
        return out_ref.at[:, pl.ds(0, count * BLOCK), :]

    def await_sent(count):
        while count > 0:
            span_bytes(rows_of(min(count, blocks)), out_sem, out_sem).wait_send()
            count -= blocks

    for m in reversed(range(n)):
        near = [o for o in range(n) if (o < half) == (m < half)]
        far = [o for o in range(n) if o not in near]
        into = near if m % 2 == 0 else list(range(n))
        received = sum(sizes[o] for o in into)
        relayed = sum(sizes[o] - direct_of[o] for o in far) if m % 2 == 0 else 0

        @pl.when(jnp.logical_and(me == m, hub))
        def _():
            await_sent(blocks + 4 * sizes[m] + 2 * direct_of[m] + relayed)
            if received > sizes[m]:
                span_bytes(rows_of(received - sizes[m]), take_sem, take_sem).wait_recv()

        @pl.when(jnp.logical_and(me == m, leaf))
        def _():
            await_sent(blocks + relayed)
            span_bytes(rows_of(received), take_sem, take_sem).wait_recv()


def fused_call(emissivity, bin_index, color_table, brick_order, n, ray_step):
    cells, cols_x, cols_y = emissivity.shape
    blocks = cols_x // BLOCK
    sizes = scaled(SIZES, blocks)
    most = max(sizes)
    crossing = max(sum(sizes[: n // 2]), sum(sizes[n // 2 :]))
    return pl.pallas_call(
        functools.partial(fused, n, ray_step),
        out_shape=pltpu.VMEM((4, cols_x, cols_y), jnp.float32),
        in_specs=[pl.BlockSpec(memory_space=pltpu.HBM)] * 4,
        out_specs=pl.BlockSpec(memory_space=pltpu.VMEM),
        scratch_shapes=[
            pltpu.VMEM((blocks, cells, BLOCK, cols_y), jnp.bfloat16),
            pltpu.VMEM((blocks, cells, BLOCK, cols_y), jnp.int32),
            pltpu.VMEM((blocks, 4, BLOCK, cols_y), jnp.float32),
            pltpu.VMEM((most, 2 * n, 4, BLOCK, cols_y), jnp.float32),
            pltpu.VMEM((2, most, 4, BLOCK, cols_y), jnp.float32),
            pltpu.VMEM(color_table.shape, color_table.dtype),
            pltpu.SMEM(brick_order.shape, brick_order.dtype),
            pltpu.SemaphoreType.DMA((GROUP,)),
            pltpu.SemaphoreType.DMA(()),
            pltpu.SemaphoreType.DMA((most,)),
            pltpu.SemaphoreType.DMA(()),
            pltpu.SemaphoreType.DMA((crossing,)),
            pltpu.SemaphoreType.REGULAR,
            pltpu.SemaphoreType.REGULAR((n,)),
        ],
        compiler_params=pltpu.CompilerParams(collective_id=0, has_side_effects=True),
    )(emissivity, bin_index, color_table, brick_order)


def march_kernel(ray_step, emis_ref, bins_ref, table_ref, out_ref):
    tables = scaled_tables(table_ref, ray_step)

    @pl.loop(0, emis_ref.shape[1] // BLOCK)
    def _(r):
        start = pl.multiple_of(r * BLOCK, BLOCK)
        part = march(tables, emis_ref, bins_ref, start)
        for c in range(4):
            out_ref[c, pl.ds(start, BLOCK), :] = part[c]


def spread(emissivity, bin_index, color_table, brick_order, n, ray_step):
    cells, cols_x, cols_y = emissivity.shape
    piece_len = cols_x * cols_y // n
    stacked = pl.pallas_call(
        functools.partial(march_kernel, ray_step),
        out_shape=jax.ShapeDtypeStruct((4, cols_x, cols_y), jnp.float32),
        in_specs=[pl.BlockSpec(memory_space=pltpu.VMEM)] * 3,
        out_specs=pl.BlockSpec(memory_space=pltpu.VMEM),
    )(emissivity, bin_index, color_table)
    stacked = stacked.reshape(1, 4, n, piece_len).transpose(2, 0, 1, 3).reshape(n, 4, piece_len)
    received = lax.all_to_all(stacked, "depth", split_axis=0, concat_axis=0, tiled=True)
    ordered = jnp.take(received, brick_order, axis=0)
    color, through = ordered[0, 0:3], ordered[0, 3]
    for k in range(1, n):
        color = color + through * ordered[k, 0:3]
        through = through * ordered[k, 3]
    piece = jnp.concatenate([color, (1.0 - through)[None]], 0)
    return lax.all_gather(piece, "depth", axis=1, tiled=True).reshape(4, cols_x, cols_y)


def on_device(emissivity, bin_index, color_table, brick_order):
    cells, cols_x, cols_y = emissivity.shape
    n = lax.axis_size("depth")
    ray_step = 2.0 / (cells * n)
    paired = lax.axis_size("imgx") % 2 == 0
    piecewise = n == len(RS) and paired and cols_x % (sum(SIZES) * BLOCK) == 0
    form = fused_call if piecewise else spread
    return form(emissivity, bin_index, color_table, brick_order, n, ray_step)


def solution(mesh):
    return jax.shard_map(
        on_device,
        mesh=mesh,
        in_specs=(P("depth", "imgx", "imgy"), P("depth", "imgx", "imgy"), P(), P()),
        out_specs=P(None, "imgx", "imgy"),
        check_vma=False,
    )
```

```python
import functools

import jax
import jax.numpy as jnp
from jax import lax
from jax.experimental import pallas as pl
from jax.experimental.pallas import tpu as pltpu
from jax.sharding import PartitionSpec as P

MESH = pl.DeviceIdType.MESH
BLOCK = 8
LANES = 128
MEET = 12
GROUP = 2
RS = (
    ((1, 0, 0.6), (2, 0.2, 1), (0, 2, 3)),
    ((2, 0, 0.9), (0, 0.5, 1), (1, 2, 3)),
    ((0, 0, 1), (1, 0, 1), (3, 1, 1.5), (2, 2, 3)),
    ((0, 0, 1), (1, 0, 0.7), (2, 0, 1), (3, 2, 3)),
)
RELAY_ORDER = ((2, 1), (3, 0))
DIRECT = (1, 0, 4, 0)
SIZES = (4, 4, 8, 0)


def look(channel_tables, bins):
    slabs = len(channel_tables[0])
    if slabs == 1:
        return [jnp.take_along_axis(t[0], bins, axis=1, mode="promise_in_bounds") for t in channel_tables]
    within = bins % LANES
    slab_of = bins // LANES
    out = []
    for t in channel_tables:
        value = jnp.take_along_axis(t[0], within, axis=1, mode="promise_in_bounds")
        for s in range(1, slabs):
            other = jnp.take_along_axis(t[s], within, axis=1, mode="promise_in_bounds")
            value = jnp.where(slab_of == s, other, value)
        out.append(value)
    return out


def scaled_tables(table_ref, ray_step):
    table = table_ref[...].astype(jnp.float32) * ray_step
    slabs = table.shape[1] // LANES
    return [
        [jnp.broadcast_to(table[c : c + 1, s * LANES : (s + 1) * LANES], (BLOCK, LANES)) for s in range(slabs)]
        for c in range(4)
    ]


def march(tables, emis_ref, bins_ref, start):
    cells = emis_ref.shape[0]
    rows = pl.ds(start, BLOCK)
    color = [None] * 3
    depth_in = None
    for z in range(cells):
        bright = emis_ref[z, rows, :].astype(jnp.float32)
        looked = look(tables, bins_ref[z, rows, :])
        rate = bright * looked[3]
        if depth_in is None:
            color = [bright * looked[c] for c in range(3)]
            depth_in = rate
        else:
            seen = bright * jnp.exp(-depth_in)
            color = [color[c] + seen * looked[c] for c in range(3)]
            depth_in = depth_in + rate
    return color + [jnp.exp(-depth_in)]


def pick(options, me):
    value = jnp.int32(options[0])
    for i in range(1, len(options)):
        value = jnp.where(me == i, jnp.int32(options[i]), value)
    return value


def scaled(shares, blocks):
    return tuple(share * blocks // sum(SIZES) for share in shares)


def owned_blocks(sizes, spans):
    steps = [(begin + (end - begin) * (k + 0.5) / sizes[o], o, k) for o, begin, end in spans for k in range(sizes[o])]
    return [(o, k) for _, o, k in sorted(steps)]


def either(me, members):
    return functools.reduce(jnp.logical_or, [me == m for m in members], False)


def fused(n, ray_step, emis_hbm, bins_hbm, table_in, order_in, out_ref,
          emis, bins, outgoing, arrived, mine, table_v, order_s, in_sem,
          out_sem, recv_sem, take_sem, cross_sem, ready_sem, know_sem):
    me = lax.axis_index("depth")
    y = lax.axis_index("imgx")
    core = lax.rem(y, 2)
    leaf, hub = core == 0, core == 1
    leaf_y, hub_y = y - core, y - core + 1
    blocks = emis.shape[0]
    half = n // 2
    sizes, direct_of = scaled(SIZES, blocks), scaled(DIRECT, blocks)
    offs = [sum(sizes[:m]) for m in range(n)]
    plan = [owned_blocks(sizes, RS[m]) for m in range(n)]

    def at_leaf(d):
        return {"depth": d, "imgx": leaf_y}

    def at_hub(d):
        return {"depth": d, "imgx": hub_y}

    barrier = pltpu.get_barrier_semaphore()

    @pl.when(hub)
    def _():
        pl.semaphore_signal(barrier, inc=1, device_id=at_leaf(me), device_id_type=MESH)
        for d in range(n):
            @pl.when((d > me) | ((d == 0) & (me == 1)))
            def _():
                pl.semaphore_signal(barrier, inc=1, device_id=at_hub(d), device_id_type=MESH)

    def block_rows(block):
        return pl.ds(pl.multiple_of(block * BLOCK, BLOCK), BLOCK)

    owner = [pick([plan[m][q][0] for m in range(n)], me) for q in range(blocks)]
    place = [pick([plan[m][q][1] for m in range(n)], me) for q in range(blocks)]
    block = [pick([offs[plan[m][q][0]] + plan[m][q][1] for m in range(n)], me) for q in range(blocks)]
    first_own = pick(offs, me)
    group = blocks // GROUP

    for q in range(blocks):
        src = block_rows(block[q])
        pltpu.make_async_copy(emis_hbm.at[:, src, :], emis.at[q], in_sem.at[q // group]).start()
        pltpu.make_async_copy(bins_hbm.at[:, src, :], bins.at[q], in_sem.at[q // group]).start()
        if q == group - 1:
            tc = pltpu.make_async_copy(table_in, table_v, in_sem.at[0])
            tc.start()
    oc = pltpu.make_async_copy(order_in, order_s, in_sem.at[GROUP - 1])
    oc.start()

    def await_group(g):
        part = pl.ds(g * group, group)
        pltpu.make_async_copy(emis.at[part], emis.at[part], in_sem.at[g]).wait()
        pltpu.make_async_copy(bins.at[part], bins.at[part], in_sem.at[g]).wait()
        if g == 0:
            tc.wait()
        if g == GROUP - 1:
            oc.wait()

    pl.semaphore_wait(barrier, jnp.where(hub, jnp.maximum(me, 1), 1))

    @pl.when(hub)
    def _():
        for d in range(n):
            @pl.when(d < me)
            def _():
                pl.semaphore_signal(know_sem.at[me], inc=1, device_id=at_hub(d), device_id_type=MESH)
        pl.semaphore_wait(know_sem.at[me], 1)
        for d in range(n):
            @pl.when(d < me)
            def _():
                pl.semaphore_signal(know_sem.at[d], inc=1, device_id=at_leaf(me), device_id_type=MESH)

    @pl.when(leaf)
    def _():
        pl.semaphore_signal(know_sem.at[me], inc=1, device_id=at_hub(me), device_id_type=MESH)

    def meet(t):
        @pl.when(jnp.logical_and(hub, t > me))
        def _():
            pl.semaphore_wait(know_sem.at[t], 1)
            pl.semaphore_signal(know_sem.at[t], inc=1, device_id=at_leaf(me), device_id_type=MESH)

        @pl.when(jnp.logical_and(leaf, t != me))
        def _():
            pl.semaphore_wait(know_sem.at[t], 1)

    await_group(0)
    tables = scaled_tables(table_v, ray_step)

    def ship(q):
        pltpu.make_async_remote_copy(
            src_ref=outgoing.at[q],
            dst_ref=arrived.at[place[q], core * n + me],
            send_sem=out_sem,
            recv_sem=recv_sem.at[place[q]],
            device_id=at_hub(owner[q]),
            device_id_type=MESH,
        ).start()

    met = [next(q for q in range(blocks) if plan[m][q][0] == o) for m in range(n) for o in range(n) if o != m and sizes[o]]
    last_meet = max(blocks * MEET // sum(SIZES), *met)
    for q in range(blocks):
        if q % group == 0 and q:
            await_group(q // group)
        got = march(tables, emis.at[q], bins.at[q], 0)
        for c in range(4):
            outgoing[q, c, :, :] = got[c]
        fresh = [m for m in range(n) if plan[m][q][0] not in [o for o, _ in plan[m][:q]]]
        if fresh:
            @pl.when(either(me, fresh))
            def _():
                meet(owner[q])
        if q == last_meet:
            for t in range(n):
                unmet = [m for m in range(n) if m != t and t not in [o for o, _ in plan[m]]]
                if unmet:
                    @pl.when(either(me, unmet))
                    def _():
                        meet(jnp.int32(t))
            @pl.when(leaf)
            def _():
                for h in range(n):
                    pl.semaphore_signal(ready_sem, inc=1, device_id=at_hub(lax.rem(me + h, n)), device_id_type=MESH)
        stays = [m for m in range(n) if plan[m][q][0] == m]
        if not stays:
            ship(q)
        else:
            here = jnp.logical_and(hub, either(me, stays))

            @pl.when(here)
            def _():
                arrived[place[q], n + me] = outgoing[q]

            @pl.when(jnp.logical_not(here))
            def _():
                ship(q)

    own_count = pick(sizes, me)
    cross = jnp.where(me < half, half, 0)
    partner = me + 1 - 2 * lax.rem(me, 2)
    cross_base = [offs[o] - offs[o // half * half] for o in range(n)]
    cross_at = pick(cross_base, me)
    direct = pick(direct_of, me)

    def span_bytes(ref, sem, other):
        return pltpu.make_async_remote_copy(src_ref=ref, dst_ref=ref, send_sem=sem, recv_sem=other, device_id=at_hub(me), device_id_type=MESH)

    def give(k, tile, d, sem):
        pltpu.make_async_remote_copy(
            src_ref=mine.at[tile, k],
            dst_ref=out_ref.at[:, block_rows(first_own + k), :],
            send_sem=out_sem,
            recv_sem=sem,
            device_id=at_leaf(d) if tile == 0 else at_hub(d),
            device_id_type=MESH,
        ).start()

    @pl.when(hub)
    def _():
        pl.semaphore_wait(ready_sem, n)
        rank = [sum(jnp.where(order_s[q] == m, q, 0) for q in range(n)) for m in range(n)]
        before = [[rank[a] < rank[b] for b in range(n)] for a in range(n)]

        def settle(k, tile):
            passed = [arrived[k, tile * n + m, 3] for m in range(n)]
            through = functools.reduce(lambda u, v: u * v, passed)
            color = [0.0] * 3
            for b in range(n):
                ahead = None
                for a in range(n):
                    if a != b:
                        factor = jnp.where(before[a][b], passed[a], 1.0)
                        ahead = factor if ahead is None else ahead * factor
                color = [color[c] + ahead * arrived[k, tile * n + b, c] for c in range(3)]
            for c in range(3):
                mine[tile, k, c] = color[c]
            mine[tile, k, 3] = 1.0 - through

        def chunk(k, carry):
            span_bytes(arrived.at[0, pl.ds(0, 2 * n - 1)], out_sem, recv_sem.at[k]).wait_recv()
            for tile in range(2):
                settle(k, tile)
                give(k, tile, cross, cross_sem.at[cross_at + k])
                give(k, tile, partner, take_sem)
                if tile == 0:
                    give(k, tile, me, take_sem)
            return carry

        lax.fori_loop(0, own_count, chunk, 0)
        if any(direct_of):
            def more(k, carry):
                for tile in range(2):
                    give(k, tile, cross + 1, take_sem)
                return carry
            lax.fori_loop(own_count - direct, own_count, more, 0)

        def keep(k, carry):
            out_ref[:, block_rows(first_own + k), :] = mine[1, k]
            return carry

        lax.fori_loop(0, own_count, keep, 0)

    even = lax.rem(me, 2) == 0

    @pl.when(even)
    def _():
        for left_far, right_far in RELAY_ORDER:
            both = (left_far, right_far)
            begin = pick([offs[left_far]] * half + [offs[right_far]] * half, me)
            count = pick([sizes[left_far]] * half + [sizes[right_far]] * half, me)
            slot = pick([cross_base[left_far]] * half + [cross_base[right_far]] * half, me)
            handed = count - pick([direct_of[left_far]] * half + [direct_of[right_far]] * half, me)

            def relay(k, carry):
                spot = out_ref.at[:, block_rows(begin + k), :]
                span_bytes(spot, out_sem, cross_sem.at[slot + k]).wait_recv()

                @pl.when(k < handed)
                def _():
                    pltpu.make_async_remote_copy(
                        src_ref=spot, dst_ref=spot, send_sem=out_sem, recv_sem=take_sem,
                        device_id={"depth": me + 1}, device_id_type=MESH).start()
                return carry

            lax.fori_loop(0, count, relay, 0)

    def rows_of(count):
        return out_ref.at[:, pl.ds(0, count * BLOCK), :]

    def await_sent(count):
        while count > 0:
            span_bytes(rows_of(min(count, blocks)), out_sem, out_sem).wait_send()
            count -= blocks

    for m in reversed(range(n)):
        near = [o for o in range(n) if (o < half) == (m < half)]
        far = [o for o in range(n) if o not in near]
        into = near if m % 2 == 0 else list(range(n))
        received = sum(sizes[o] for o in into)
        relayed = sum(sizes[o] - direct_of[o] for o in far) if m % 2 == 0 else 0

        @pl.when(jnp.logical_and(me == m, hub))
        def _():
            await_sent(blocks + 4 * sizes[m] + 2 * direct_of[m] + relayed)
            if received > sizes[m]:
                span_bytes(rows_of(received - sizes[m]), take_sem, take_sem).wait_recv()

        @pl.when(jnp.logical_and(me == m, leaf))
        def _():
            await_sent(blocks + relayed)
            span_bytes(rows_of(received), take_sem, take_sem).wait_recv()


def fused_call(emissivity, bin_index, color_table, brick_order, n, ray_step):
    cells, cols_x, cols_y = emissivity.shape
    blocks = cols_x // BLOCK
    sizes = scaled(SIZES, blocks)
    most = max(sizes)
    crossing = max(sum(sizes[: n // 2]), sum(sizes[n // 2 :]))
    return pl.pallas_call(
        functools.partial(fused, n, ray_step),
        out_shape=pltpu.VMEM((4, cols_x, cols_y), jnp.float32),
        in_specs=[pl.BlockSpec(memory_space=pltpu.HBM)] * 4,
        out_specs=pl.BlockSpec(memory_space=pltpu.VMEM),
        scratch_shapes=[
            pltpu.VMEM((blocks, cells, BLOCK, cols_y), jnp.bfloat16),
            pltpu.VMEM((blocks, cells, BLOCK, cols_y), jnp.int32),
            pltpu.VMEM((blocks, 4, BLOCK, cols_y), jnp.float32),
            pltpu.VMEM((most, 2 * n, 4, BLOCK, cols_y), jnp.float32),
            pltpu.VMEM((2, most, 4, BLOCK, cols_y), jnp.float32),
            pltpu.VMEM(color_table.shape, color_table.dtype),
            pltpu.SMEM(brick_order.shape, brick_order.dtype),
            pltpu.SemaphoreType.DMA((GROUP,)),
            pltpu.SemaphoreType.DMA(()),
            pltpu.SemaphoreType.DMA((most,)),
            pltpu.SemaphoreType.DMA(()),
            pltpu.SemaphoreType.DMA((crossing,)),
            pltpu.SemaphoreType.REGULAR,
            pltpu.SemaphoreType.REGULAR((n,)),
        ],
        compiler_params=pltpu.CompilerParams(collective_id=0, has_side_effects=True),
    )(emissivity, bin_index, color_table, brick_order)


def march_kernel(ray_step, emis_ref, bins_ref, table_ref, out_ref):
    tables = scaled_tables(table_ref, ray_step)

    @pl.loop(0, emis_ref.shape[1] // BLOCK)
    def _(r):
        start = pl.multiple_of(r * BLOCK, BLOCK)
        part = march(tables, emis_ref, bins_ref, start)
        for c in range(4):
            out_ref[c, pl.ds(start, BLOCK), :] = part[c]


def spread(emissivity, bin_index, color_table, brick_order, n, ray_step):
    cells, cols_x, cols_y = emissivity.shape
    piece_len = cols_x * cols_y // n
    stacked = pl.pallas_call(
        functools.partial(march_kernel, ray_step),
        out_shape=jax.ShapeDtypeStruct((4, cols_x, cols_y), jnp.float32),
        in_specs=[pl.BlockSpec(memory_space=pltpu.VMEM)] * 3,
        out_specs=pl.BlockSpec(memory_space=pltpu.VMEM),
    )(emissivity, bin_index, color_table)
    stacked = stacked.reshape(1, 4, n, piece_len).transpose(2, 0, 1, 3).reshape(n, 4, piece_len)
    received = lax.all_to_all(stacked, "depth", split_axis=0, concat_axis=0, tiled=True)
    ordered = jnp.take(received, brick_order, axis=0)
    color, through = ordered[0, 0:3], ordered[0, 3]
    for k in range(1, n):
        color = color + through * ordered[k, 0:3]
        through = through * ordered[k, 3]
    piece = jnp.concatenate([color, (1.0 - through)[None]], 0)
    return lax.all_gather(piece, "depth", axis=1, tiled=True).reshape(4, cols_x, cols_y)


def on_device(emissivity, bin_index, color_table, brick_order):
    cells, cols_x, cols_y = emissivity.shape
    n = lax.axis_size("depth")
    ray_step = 2.0 / (cells * n)
    paired = lax.axis_size("imgx") % 2 == 0
    piecewise = n == len(RS) and paired and cols_x % (sum(SIZES) * BLOCK) == 0
    form = fused_call if piecewise else spread
    return form(emissivity, bin_index, color_table, brick_order, n, ray_step)


def solution(mesh):
    return jax.shard_map(
        on_device,
        mesh=mesh,
        in_specs=(P("depth", "imgx", "imgy"), P("depth", "imgx", "imgy"), P(), P()),
        out_specs=P(None, "imgx", "imgy"),
        check_vma=False,
    )
```

```python
import functools

import jax
import jax.numpy as jnp
from jax import lax
from jax.experimental import pallas as pl
from jax.experimental.pallas import tpu as pltpu
from jax.sharding import PartitionSpec as P

MESH = pl.DeviceIdType.MESH
BLOCK = 8
LANES = 128
MEET = 12
GROUP = 2
RS = (
    ((1, 0, 0.6), (2, 0.2, 1), (0, 2, 3)),
    ((2, 0, 0.9), (0, 0.5, 1), (1, 2, 3)),
    ((0, 0, 1), (1, 0, 1), (3, 1, 1.5), (2, 2, 3)),
    ((0, 0, 1), (1, 0, 0.7), (2, 0, 1), (3, 2, 3)),
)
RELAY_ORDER = ((2, 1), (3, 0))
DIRECT = (2, 0, 4, 0)
SIZES = (4, 4, 8, 0)


def look(channel_tables, bins):
    slabs = len(channel_tables[0])
    if slabs == 1:
        return [jnp.take_along_axis(t[0], bins, axis=1, mode="promise_in_bounds") for t in channel_tables]
    within = bins % LANES
    slab_of = bins // LANES
    out = []
    for t in channel_tables:
        value = jnp.take_along_axis(t[0], within, axis=1, mode="promise_in_bounds")
        for s in range(1, slabs):
            other = jnp.take_along_axis(t[s], within, axis=1, mode="promise_in_bounds")
            value = jnp.where(slab_of == s, other, value)
        out.append(value)
    return out


def scaled_tables(table_ref, ray_step):
    table = table_ref[...].astype(jnp.float32) * ray_step
    slabs = table.shape[1] // LANES
    return [
        [jnp.broadcast_to(table[c : c + 1, s * LANES : (s + 1) * LANES], (BLOCK, LANES)) for s in range(slabs)]
        for c in range(4)
    ]


def march(tables, emis_ref, bins_ref, start):
    cells = emis_ref.shape[0]
    rows = pl.ds(start, BLOCK)
    color = [None] * 3
    depth_in = None
    for z in range(cells):
        bright = emis_ref[z, rows, :].astype(jnp.float32)
        looked = look(tables, bins_ref[z, rows, :])
        rate = bright * looked[3]
        if depth_in is None:
            color = [bright * looked[c] for c in range(3)]
            depth_in = rate
        else:
            seen = bright * jnp.exp(-depth_in)
            color = [color[c] + seen * looked[c] for c in range(3)]
            depth_in = depth_in + rate
    return color + [jnp.exp(-depth_in)]


def pick(options, me):
    value = jnp.int32(options[0])
    for i in range(1, len(options)):
        value = jnp.where(me == i, jnp.int32(options[i]), value)
    return value


def scaled(shares, blocks):
    return tuple(share * blocks // sum(SIZES) for share in shares)


def owned_blocks(sizes, spans):
    steps = [(begin + (end - begin) * (k + 0.5) / sizes[o], o, k) for o, begin, end in spans for k in range(sizes[o])]
    return [(o, k) for _, o, k in sorted(steps)]


def either(me, members):
    return functools.reduce(jnp.logical_or, [me == m for m in members], False)


def fused(n, ray_step, emis_hbm, bins_hbm, table_in, order_in, out_ref,
          emis, bins, outgoing, arrived, mine, table_v, order_s, in_sem,
          out_sem, recv_sem, take_sem, cross_sem, ready_sem, know_sem):
    me = lax.axis_index("depth")
    y = lax.axis_index("imgx")
    core = lax.rem(y, 2)
    leaf, hub = core == 0, core == 1
    leaf_y, hub_y = y - core, y - core + 1
    blocks = emis.shape[0]
    half = n // 2
    sizes, direct_of = scaled(SIZES, blocks), scaled(DIRECT, blocks)
    offs = [sum(sizes[:m]) for m in range(n)]
    plan = [owned_blocks(sizes, RS[m]) for m in range(n)]

    def at_leaf(d):
        return {"depth": d, "imgx": leaf_y}

    def at_hub(d):
        return {"depth": d, "imgx": hub_y}

    barrier = pltpu.get_barrier_semaphore()

    @pl.when(hub)
    def _():
        pl.semaphore_signal(barrier, inc=1, device_id=at_leaf(me), device_id_type=MESH)
        for d in range(n):
            @pl.when((d > me) | ((d == 0) & (me == 1)))
            def _():
                pl.semaphore_signal(barrier, inc=1, device_id=at_hub(d), device_id_type=MESH)

    def block_rows(block):
        return pl.ds(pl.multiple_of(block * BLOCK, BLOCK), BLOCK)

    owner = [pick([plan[m][q][0] for m in range(n)], me) for q in range(blocks)]
    place = [pick([plan[m][q][1] for m in range(n)], me) for q in range(blocks)]
    block = [pick([offs[plan[m][q][0]] + plan[m][q][1] for m in range(n)], me) for q in range(blocks)]
    first_own = pick(offs, me)
    group = blocks // GROUP

    for q in range(blocks):
        src = block_rows(block[q])
        pltpu.make_async_copy(emis_hbm.at[:, src, :], emis.at[q], in_sem.at[q // group]).start()
        pltpu.make_async_copy(bins_hbm.at[:, src, :], bins.at[q], in_sem.at[q // group]).start()
        if q == group - 1:
            tc = pltpu.make_async_copy(table_in, table_v, in_sem.at[0])
            tc.start()
    oc = pltpu.make_async_copy(order_in, order_s, in_sem.at[GROUP - 1])
    oc.start()

    def await_group(g):
        part = pl.ds(g * group, group)
        pltpu.make_async_copy(emis.at[part], emis.at[part], in_sem.at[g]).wait()
        pltpu.make_async_copy(bins.at[part], bins.at[part], in_sem.at[g]).wait()
        if g == 0:
            tc.wait()
        if g == GROUP - 1:
            oc.wait()

    pl.semaphore_wait(barrier, jnp.where(hub, jnp.maximum(me, 1), 1))

    @pl.when(hub)
    def _():
        for d in range(n):
            @pl.when(d < me)
            def _():
                pl.semaphore_signal(know_sem.at[me], inc=1, device_id=at_hub(d), device_id_type=MESH)
        pl.semaphore_wait(know_sem.at[me], 1)
        for d in range(n):
            @pl.when(d < me)
            def _():
                pl.semaphore_signal(know_sem.at[d], inc=1, device_id=at_leaf(me), device_id_type=MESH)

    @pl.when(leaf)
    def _():
        pl.semaphore_signal(know_sem.at[me], inc=1, device_id=at_hub(me), device_id_type=MESH)

    def meet(t):
        @pl.when(jnp.logical_and(hub, t > me))
        def _():
            pl.semaphore_wait(know_sem.at[t], 1)
            pl.semaphore_signal(know_sem.at[t], inc=1, device_id=at_leaf(me), device_id_type=MESH)

        @pl.when(jnp.logical_and(leaf, t != me))
        def _():
            pl.semaphore_wait(know_sem.at[t], 1)

    await_group(0)
    tables = scaled_tables(table_v, ray_step)

    def ship(q):
        pltpu.make_async_remote_copy(
            src_ref=outgoing.at[q],
            dst_ref=arrived.at[place[q], core * n + me],
            send_sem=out_sem,
            recv_sem=recv_sem.at[place[q]],
            device_id=at_hub(owner[q]),
            device_id_type=MESH,
        ).start()

    met = [next(q for q in range(blocks) if plan[m][q][0] == o) for m in range(n) for o in range(n) if o != m and sizes[o]]
    last_meet = max(blocks * MEET // sum(SIZES), *met)
    for q in range(blocks):
        if q % group == 0 and q:
            await_group(q // group)
        got = march(tables, emis.at[q], bins.at[q], 0)
        for c in range(4):
            outgoing[q, c, :, :] = got[c]
        fresh = [m for m in range(n) if plan[m][q][0] not in [o for o, _ in plan[m][:q]]]
        if fresh:
            @pl.when(either(me, fresh))
            def _():
                meet(owner[q])
        if q == last_meet:
            for t in range(n):
                unmet = [m for m in range(n) if m != t and t not in [o for o, _ in plan[m]]]
                if unmet:
                    @pl.when(either(me, unmet))
                    def _():
                        meet(jnp.int32(t))
            @pl.when(leaf)
            def _():
                for h in range(n):
                    pl.semaphore_signal(ready_sem, inc=1, device_id=at_hub(lax.rem(me + h, n)), device_id_type=MESH)
        stays = [m for m in range(n) if plan[m][q][0] == m]
        if not stays:
            ship(q)
        else:
            here = jnp.logical_and(hub, either(me, stays))

            @pl.when(here)
            def _():
                arrived[place[q], n + me] = outgoing[q]

            @pl.when(jnp.logical_not(here))
            def _():
                ship(q)

    own_count = pick(sizes, me)
    cross = jnp.where(me < half, half, 0)
    partner = me + 1 - 2 * lax.rem(me, 2)
    cross_base = [offs[o] - offs[o // half * half] for o in range(n)]
    cross_at = pick(cross_base, me)
    direct = pick(direct_of, me)

    def span_bytes(ref, sem, other):
        return pltpu.make_async_remote_copy(src_ref=ref, dst_ref=ref, send_sem=sem, recv_sem=other, device_id=at_hub(me), device_id_type=MESH)

    def give(k, tile, d, sem):
        pltpu.make_async_remote_copy(
            src_ref=mine.at[tile, k],
            dst_ref=out_ref.at[:, block_rows(first_own + k), :],
            send_sem=out_sem,
            recv_sem=sem,
            device_id=at_leaf(d) if tile == 0 else at_hub(d),
            device_id_type=MESH,
        ).start()

    @pl.when(hub)
    def _():
        pl.semaphore_wait(ready_sem, n)
        rank = [sum(jnp.where(order_s[q] == m, q, 0) for q in range(n)) for m in range(n)]
        before = [[rank[a] < rank[b] for b in range(n)] for a in range(n)]

        def settle(k, tile):
            passed = [arrived[k, tile * n + m, 3] for m in range(n)]
            through = functools.reduce(lambda u, v: u * v, passed)
            color = [0.0] * 3
            for b in range(n):
                ahead = None
                for a in range(n):
                    if a != b:
                        factor = jnp.where(before[a][b], passed[a], 1.0)
                        ahead = factor if ahead is None else ahead * factor
                color = [color[c] + ahead * arrived[k, tile * n + b, c] for c in range(3)]
            for c in range(3):
                mine[tile, k, c] = color[c]
            mine[tile, k, 3] = 1.0 - through

        def chunk(k, carry):
            span_bytes(arrived.at[0, pl.ds(0, 2 * n - 1)], out_sem, recv_sem.at[k]).wait_recv()
            for tile in range(2):
                settle(k, tile)
                give(k, tile, cross, cross_sem.at[lax.div(cross_at + k, 2)])
                give(k, tile, partner, take_sem)
                if tile == 0:
                    give(k, tile, me, take_sem)
            return carry

        lax.fori_loop(0, own_count, chunk, 0)
        if any(direct_of):
            def more(k, carry):
                for tile in range(2):
                    give(k, tile, cross + 1, take_sem)
                return carry
            lax.fori_loop(own_count - direct, own_count, more, 0)

        def keep(k, carry):
            out_ref[:, block_rows(first_own + k), :] = mine[1, k]
            return carry

        lax.fori_loop(0, own_count, keep, 0)

    even = lax.rem(me, 2) == 0

    @pl.when(even)
    def _():
        for left_far, right_far in RELAY_ORDER:
            both = (left_far, right_far)
            begin = pick([offs[left_far]] * half + [offs[right_far]] * half, me)
            count = pick([sizes[left_far]] * half + [sizes[right_far]] * half, me)
            slot = pick([cross_base[left_far]] * half + [cross_base[right_far]] * half, me)
            handed = count - pick([direct_of[left_far]] * half + [direct_of[right_far]] * half, me)

            def relay(k, carry):
                spot = out_ref.at[:, pl.ds(pl.multiple_of((begin + 2 * k) * BLOCK, BLOCK), 2 * BLOCK), :]
                span_bytes(spot, out_sem, cross_sem.at[lax.div(slot, 2) + k]).wait_recv()

                @pl.when(2 * k < handed)
                def _():
                    pltpu.make_async_remote_copy(
                        src_ref=spot, dst_ref=spot, send_sem=out_sem, recv_sem=take_sem,
                        device_id={"depth": me + 1}, device_id_type=MESH).start()
                return carry

            lax.fori_loop(0, lax.div(count, 2), relay, 0)

    def rows_of(count):
        return out_ref.at[:, pl.ds(0, count * BLOCK), :]

    def await_sent(count):
        while count > 0:
            span_bytes(rows_of(min(count, blocks)), out_sem, out_sem).wait_send()
            count -= blocks

    for m in reversed(range(n)):
        near = [o for o in range(n) if (o < half) == (m < half)]
        far = [o for o in range(n) if o not in near]
        into = near if m % 2 == 0 else list(range(n))
        received = sum(sizes[o] for o in into)
        relayed = sum(sizes[o] - direct_of[o] for o in far) if m % 2 == 0 else 0

        @pl.when(jnp.logical_and(me == m, hub))
        def _():
            await_sent(blocks + 4 * sizes[m] + 2 * direct_of[m] + relayed)
            if received > sizes[m]:
                span_bytes(rows_of(received - sizes[m]), take_sem, take_sem).wait_recv()

        @pl.when(jnp.logical_and(me == m, leaf))
        def _():
            await_sent(blocks + relayed)
            span_bytes(rows_of(received), take_sem, take_sem).wait_recv()


def fused_call(emissivity, bin_index, color_table, brick_order, n, ray_step):
    cells, cols_x, cols_y = emissivity.shape
    blocks = cols_x // BLOCK
    sizes = scaled(SIZES, blocks)
    most = max(sizes)
    crossing = max(sum(sizes[: n // 2]), sum(sizes[n // 2 :]))
    return pl.pallas_call(
        functools.partial(fused, n, ray_step),
        out_shape=pltpu.VMEM((4, cols_x, cols_y), jnp.float32),
        in_specs=[pl.BlockSpec(memory_space=pltpu.HBM)] * 4,
        out_specs=pl.BlockSpec(memory_space=pltpu.VMEM),
        scratch_shapes=[
            pltpu.VMEM((blocks, cells, BLOCK, cols_y), jnp.bfloat16),
            pltpu.VMEM((blocks, cells, BLOCK, cols_y), jnp.int32),
            pltpu.VMEM((blocks, 4, BLOCK, cols_y), jnp.float32),
            pltpu.VMEM((most, 2 * n, 4, BLOCK, cols_y), jnp.float32),
            pltpu.VMEM((2, most, 4, BLOCK, cols_y), jnp.float32),
            pltpu.VMEM(color_table.shape, color_table.dtype),
            pltpu.SMEM(brick_order.shape, brick_order.dtype),
            pltpu.SemaphoreType.DMA((GROUP,)),
            pltpu.SemaphoreType.DMA(()),
            pltpu.SemaphoreType.DMA((most,)),
            pltpu.SemaphoreType.DMA(()),
            pltpu.SemaphoreType.DMA((crossing // 2,)),
            pltpu.SemaphoreType.REGULAR,
            pltpu.SemaphoreType.REGULAR((n,)),
        ],
        compiler_params=pltpu.CompilerParams(collective_id=0, has_side_effects=True),
    )(emissivity, bin_index, color_table, brick_order)


def march_kernel(ray_step, emis_ref, bins_ref, table_ref, out_ref):
    tables = scaled_tables(table_ref, ray_step)

    @pl.loop(0, emis_ref.shape[1] // BLOCK)
    def _(r):
        start = pl.multiple_of(r * BLOCK, BLOCK)
        part = march(tables, emis_ref, bins_ref, start)
        for c in range(4):
            out_ref[c, pl.ds(start, BLOCK), :] = part[c]


def spread(emissivity, bin_index, color_table, brick_order, n, ray_step):
    cells, cols_x, cols_y = emissivity.shape
    piece_len = cols_x * cols_y // n
    stacked = pl.pallas_call(
        functools.partial(march_kernel, ray_step),
        out_shape=jax.ShapeDtypeStruct((4, cols_x, cols_y), jnp.float32),
        in_specs=[pl.BlockSpec(memory_space=pltpu.VMEM)] * 3,
        out_specs=pl.BlockSpec(memory_space=pltpu.VMEM),
    )(emissivity, bin_index, color_table)
    stacked = stacked.reshape(1, 4, n, piece_len).transpose(2, 0, 1, 3).reshape(n, 4, piece_len)
    received = lax.all_to_all(stacked, "depth", split_axis=0, concat_axis=0, tiled=True)
    ordered = jnp.take(received, brick_order, axis=0)
    color, through = ordered[0, 0:3], ordered[0, 3]
    for k in range(1, n):
        color = color + through * ordered[k, 0:3]
        through = through * ordered[k, 3]
    piece = jnp.concatenate([color, (1.0 - through)[None]], 0)
    return lax.all_gather(piece, "depth", axis=1, tiled=True).reshape(4, cols_x, cols_y)


def on_device(emissivity, bin_index, color_table, brick_order):
    cells, cols_x, cols_y = emissivity.shape
    n = lax.axis_size("depth")
    ray_step = 2.0 / (cells * n)
    paired = lax.axis_size("imgx") % 2 == 0
    piecewise = n == len(RS) and paired and cols_x % (sum(SIZES) * BLOCK) == 0
    form = fused_call if piecewise else spread
    return form(emissivity, bin_index, color_table, brick_order, n, ray_step)


def solution(mesh):
    return jax.shard_map(
        on_device,
        mesh=mesh,
        in_specs=(P("depth", "imgx", "imgy"), P("depth", "imgx", "imgy"), P(), P()),
        out_specs=P(None, "imgx", "imgy"),
        check_vma=False,
    )
```
